256 devices in a mesh: row: 32 (over x, z), col: 8 (over y, core).
Axes of the slice: x: 4, y: 4, z: 8, core: 2. Of those that a mesh axis runs over, the one named last changes fastest.
Arguments:
- matrix: float32 [5, 32, 20, 8, 128, 128], P(None, 'row', None, 'col'), may hold values from 0 to 2.5, as said below
- flags: int32 [5, 32, 20, 8], P(None, 'row', None, 'col'), may hold values from 0 to 1, as said below
Outputs:
- factor: float32 [5, 32, 20, 8, 128, 128], P(None, 'row', None, 'col')
The draws below stay inside these ranges and needn't reach their ends.
Inputs may be any that keep to these rules, and one draw needn't show every extreme that they name: `matrix`: symmetric positive definite, of order 160*128, diagonal at least 1.5. `flags`: 0 marks a float32 tile, 1 a bfloat16 tile; every diagonal tile is 0.
All inputs are finite; a program needn't handle non-finite values.
Results may differ from the reference program's by a relative error of at most 0.0005.
The reference program's roundings to bfloat16 on the way count: a program that leaves them out, or rounds other values in their place, can miss the bound.
Values sent between devices are 32-bit elements; how exact they have to be, the bound alone decides.
A program may use at most 128 MiB of HBM per device.

```python
import jax
import jax.numpy as jnp
from jax import lax

B = 128
PT = 4
TR_DEV = 5
NT = 160
TC_DEV = 20


def draw_matrix(key, part):
    count = NT * B
    points = jax.random.uniform(jax.random.fold_in(key, 11), (count, 2), jnp.float32)
    order = jnp.argsort(points[:, 0])
    points = points[order]
    reach = 0.6
    nugget = 0.5
    delta_x = points[:, 0][:, None] - points[:, 0][None, :]
    delta_y = points[:, 1][:, None] - points[:, 1][None, :]
    dist = jnp.sqrt(delta_x * delta_x + delta_y * delta_y)
    cov = jnp.exp(-dist / reach) + nugget * jnp.eye(count, dtype=jnp.float32)
    tiled = cov.reshape(NT, B, NT, B).transpose(0, 2, 1, 3)
    return tiled.reshape(TR_DEV, NT // TR_DEV, TC_DEV, NT // TC_DEV, B, B)


def draw_flags(key, part):
    tile_ids = jnp.arange(NT, dtype=jnp.int32)
    spacing = jnp.abs(tile_ids[:, None] - tile_ids[None, :])
    band = jax.random.randint(jax.random.fold_in(key, 5), (), 2, 6)
    flips = jax.random.randint(jax.random.fold_in(key, 7), (NT, NT), 0, 4)
    far_mark = (flips != 0).astype(jnp.int32)
    near_mark = (flips == 0).astype(jnp.int32)
    marks = jnp.where(spacing == 0, 0, jnp.where(spacing >= band, far_mark, near_mark))
    return marks.astype(jnp.int32).reshape(TR_DEV, NT // TR_DEV, TC_DEV, NT // TC_DEV)


def setup_inputs(seed: int = 0) -> dict:
    key_list = jax.random.split(jax.random.key(seed), 3)
    matrix = draw_matrix(jax.random.fold_in(key_list[2], 71), 0)
    flags = draw_flags(jax.random.fold_in(key_list[2], 71), 0)
    return {"matrix": matrix, "flags": flags}


def storage_round(values):
    narrow = lax.optimization_barrier(values.astype(jnp.bfloat16))
    return narrow.astype(jnp.float32)

def reference(matrix, flags):
    width = PT * B
    tiles = matrix.reshape(NT, NT, B, B)
    marks = flags.reshape(NT, NT)
    work = jnp.where((marks == 1)[:, :, None, None], storage_round(tiles), tiles)
    tile_ids = jnp.arange(NT, dtype=jnp.int32)
    for step in range(2):
        start = step * PT
        rows = work[:, start:start + PT].transpose(0, 2, 1, 3).reshape(NT, B, width)
        dense = rows[start:start + PT].reshape(width, width)
        sym = jnp.tril(dense) + jnp.tril(dense, -1).T
        lower_block = jnp.linalg.cholesky(sym)
        flat = rows.reshape(NT * B, width)
        solved = jax.scipy.linalg.solve_triangular(lower_block, flat.T, lower=True).T.reshape(NT, B, width)
        solved = solved.at[start:start + PT].set(lower_block.reshape(PT, B, width))
        rounded = storage_round(solved)

        def row_update(args):
            tile_row, mark_row, index = args
            exact = jnp.einsum('ik,cjk->cij', solved[index], solved, precision=lax.Precision.HIGHEST)
            coarse = jnp.einsum('ik,cjk->cij', rounded[index], rounded, precision=lax.Precision.HIGHEST)
            live = (index >= tile_ids) & (tile_ids >= start + PT)
            updated = jnp.where((mark_row == 1)[:, None, None], tile_row - coarse, tile_row - exact)
            return jnp.where(live[:, None, None], updated, tile_row)
        work = lax.map(row_update, (work, marks, tile_ids))
        new_cols = solved.reshape(NT, B, PT, B).transpose(0, 2, 1, 3)
        keep = (tile_ids >= start)[:, None, None, None]
        work = work.at[:, start:start + PT].set(jnp.where(keep, new_cols, work[:, start:start + PT]))
    final = jnp.where((marks == 1)[:, :, None, None], storage_round(work), work)
    upper = tile_ids[:, None] < tile_ids[None, :]
    final = jnp.where(upper[:, :, None, None], jnp.float32(0.0), final)
    return final.reshape(TR_DEV, NT // TR_DEV, TC_DEV, NT // TC_DEV, B, B)
```

```python
import jax
import jax.numpy as jnp
from jax import lax
from jax.experimental import pallas as pl
from jax.experimental.pallas import tpu as pltpu
from jax.sharding import Mesh
from jax.sharding import PartitionSpec as P

F32 = jnp.float32
BF16 = jnp.bfloat16
MESH = pl.DeviceIdType.MESH
PT = 4
HI = lax.Precision.HIGHEST
SUB = 32

def halves(v):
    high = v.astype(BF16)
    return high, (v - high.astype(F32)).astype(BF16)

NT = (((1,), (1,)), ((), ()))
TN = (((0,), (0,)), ((), ()))
NN = (((1,), (0,)), ((), ()))

def mm(a, b, dims):
    return lax.dot_general(a, b, dims, preferred_element_type=F32)

def mm3(a, b, dims):
    return mm(a[0], b[0], dims) + (mm(a[0], b[1], dims) + mm(a[1], b[0], dims))

def small_inverse(block, first):
    lanes = block.shape[1]
    cols = []
    for k in range(SUB):
        low = 8 * (k // 8)
        cols.append(jnp.broadcast_to(block[low:, first + k:first + k + 1], (SUB - low, lanes)))
    row = lax.broadcasted_iota(jnp.int32, (SUB, lanes), 0)
    lane = lax.broadcasted_iota(jnp.int32, (SUB, lanes), 1)
    right = (row == lane).astype(F32)
    done = []
    for k in range(SUB):
        low = 8 * (k // 8)
        own = cols[k]
        scale = lax.rsqrt(own[k - low:k - low + 1, :])
        factor = own * scale
        solved = right[k - low:k - low + 1, :] * scale
        done.append(solved)
        if k == SUB - 1:
            break
        nxt = 8 * ((k + 1) // 8)
        for m in range(k + 1, SUB):
            base = 8 * (m // 8)
            cols[m] = cols[m] - factor[base - low:, :] * factor[m - low:m - low + 1, :]
        right = right[nxt - low:, :] - factor[nxt - low:, :] * solved
    return jnp.concatenate(done, axis=0)

def factor_block(a_ref, u_ref, w_ref, t_ref):
    n = a_ref.shape[0]
    u_ref[...] = jnp.zeros_like(u_ref)
    w_ref[...] = jnp.zeros_like(w_ref)

    def body(kb, carry):
        here = pl.ds(pl.multiple_of(kb * 128, 128), 128)
        row = lax.broadcasted_iota(jnp.int32, (128, n), 0)
        lane = lax.broadcasted_iota(jnp.int32, (128, n), 1)
        t_ref[:, :n] = a_ref[here, :]
        t_ref[:, n:] = (lane == row + kb * 128).astype(F32)

        @pl.when(kb > 0)
        def _():
            left = halves(u_ref[:, here])
            t_ref[:, :n] -= mm3(left, halves(u_ref[...]), TN)
            t_ref[:, n:] -= mm3(left, halves(w_ref[...]), TN)

        for s in range(128 // SUB):
            rows = slice(s * SUB, (s + 1) * SUB)
            inv = small_inverse(t_ref[rows, here], s * SUB)[:, :SUB]
            both = lax.dot_general(inv, t_ref[rows, :], NN, precision=HI, preferred_element_type=F32)
            out = pl.ds(pl.multiple_of(kb * 128 + s * SUB, SUB), SUB)
            lane2 = lax.broadcasted_iota(jnp.int32, (SUB, n), 1)
            row2 = lax.broadcasted_iota(jnp.int32, (SUB, n), 0) + (kb * 128 + s * SUB)
            u_ref[out, :] = jnp.where(lane2 >= row2, both[:, :n], 0.0)
            w_ref[out, :] = jnp.where(lane2 <= row2, both[:, n:], 0.0)
            if s < 128 // SUB - 1:
                rest = slice((s + 1) * SUB, 128)
                left = halves(u_ref[out, here])
                t_ref[rest, :] -= mm3(left, halves(both), TN)[rest, :]
        return carry

    lax.fori_loop(0, n // 128, body, 0)

NX, NZ, NY, NA, NTC = 4, 8, 4, 5, 8
PR = 136
ZL, RL, FL = 1, 3, 6

def comm_kernel(pay_ref, left, right, lead, ls, lr, zs, xs, rs, rr, ds, dr):
    x, z, y, c = (lax.axis_index(n) for n in ("x", "z", "y", "c"))
    q = 2 * y + c
    xp, xm = lax.rem(x + 1, NX), lax.rem(x + NX - 1, NX)
    zp, zm = lax.rem(z + 1, NZ), lax.rem(z + NZ - 1, NZ)
    yp, ym, yo = lax.rem(y + 1, NY), lax.rem(y + NY - 1, NY), lax.rem(y + 2, NY)

    def to(src, dst, send, recv, where):
        return pltpu.make_async_remote_copy(src_ref=src, dst_ref=dst, send_sem=send, recv_sem=recv,
                                            device_id=where, device_id_type=MESH)

    barrier = pltpu.get_barrier_semaphore()
    peers = [{"x": xp}, {"x": xm}, {"z": zp}, {"z": zm}, {"y": yp}, {"y": ym}, {"c": 1 - c}]
    for p in peers:
        pl.semaphore_signal(barrier, inc=1, device_id=p, device_id_type=MESH)
    pl.semaphore_wait(barrier, len(peers))

    def group_gather(src, slot, send, recv):
        def go(k, i, ref, where):
            to(ref, slot(k), send(k, i), recv(k), where).start()
        def got(k):
            to(src, slot(k), send(k, 0), recv(k), {"c": 1 - c}).wait_recv()
        go(q, 0, src, {"y": yp})
        go(q, 1, src, {"y": ym})
        go(q, 2, src, {"c": 1 - c})
        km, kp, ko = 2 * ym + c, 2 * yp + c, 2 * yo + c
        got(km)
        @pl.when(c == 0)
        def _():
            go(km, 0, slot(km), {"y": yp})
        go(km, 2, slot(km), {"c": 1 - c})
        got(kp)
        @pl.when(c == 1)
        def _():
            go(kp, 0, slot(kp), {"y": ym})
        go(kp, 2, slot(kp), {"c": 1 - c})
        got(ko)
        go(ko, 2, slot(ko), {"c": 1 - c})
        for k in range(NY):
            got(2 * k + 1 - c)

    def group_sent(src, slot, send):
        def sent(k, i):
            to(src, slot(k), send(k, i), send(k, i), {"c": 1 - c}).wait_send()
        km, kp, ko = 2 * ym + c, 2 * yp + c, 2 * yo + c
        for i in range(3):
            sent(q, i)
        @pl.when(c == 0)
        def _():
            sent(km, 0)
        @pl.when(c == 1)
        def _():
            sent(kp, 0)
        for k in (km, kp, ko):
            sent(k, 2)

    left_args = (pay_ref, lambda k: left.at[k], lambda k, i: ls.at[k, i])
    group_gather(*left_args, lambda k: lr.at[k])
    left[pl.ds(q, 1)] = pay_ref[...][None]

    @pl.when(z == q)
    def _():
        right[pl.ds(x, 1)] = left[...][None]

    zd = (lax.rem(z - q + NZ, NZ), lax.rem(q - z + NZ, NZ))
    znext = ({"z": zp}, {"z": zm})
    xnext = ({"x": xp}, {"x": xm})
    xprev = (xm, xp)
    xfar = lax.rem(x + 2, NX)

    def piece(par, n):
        return 2 * lax.rem(n, 4) + par, n // 4

    def landed(src, t, a):
        r = right.at[src, t, a]
        to(r, r, rs.at[t, a, 0], rr.at[src, t, a], {"x": xp}).wait_recv()

    def push(src, t, a, send, where):
        r = right.at[src, t, a]
        to(r, r, send, rr.at[src, t, a], where).start()

    def step(m, carry):
        for par in range(2):
            n = m - zd[par] * ZL
            @pl.when((n >= 0) & (n < 4 * NA))
            def _():
                t, a = piece(par, n)
                @pl.when(zd[par] > 0)
                def _():
                    landed(x, t, a)
                @pl.when(zd[par] < NZ - 1)
                def _():
                    push(x, t, a, zs.at[t, a], znext[par])
                push(x, t, a, xs.at[t, a, 0], {"x": xp})
                push(x, t, a, xs.at[t, a, 1], {"x": xm})
        for par in range(2):
            n = m - zd[par] * ZL - RL
            @pl.when((n >= 0) & (n < 4 * NA))
            def _():
                t, a = piece(par, n)
                landed(xprev[par], t, a)
                push(xprev[par], t, a, rs.at[t, a, 0], xnext[par])
        for par in range(2):
            n = m - zd[par] * ZL - FL
            @pl.when((n >= 0) & (n < 4 * NA))
            def _():
                t, a = piece(par, n)
                landed(xprev[1 - par], t, a)
                landed(xfar, t, a)
        return carry

    split = 4 + 7 * ZL + FL
    last = 4 * NA + 7 * ZL + FL
    lax.fori_loop(0, split, step, 0)

    row = right.at[0, :, 0]
    lead_args = (row, lambda k: lead.at[k], lambda k, i: ds.at[k, i])
    group_gather(*lead_args, lambda k: dr.at[k])
    lead[pl.ds(q, 1)] = right[0, :, 0][None]
    lax.fori_loop(split, last, step, 0)

    group_sent(pay_ref, left_args[1], left_args[2])
    group_sent(row, lead_args[1], lead_args[2])

    def drain(n, carry):
        for par in range(2):
            t, a = piece(par, n)
            r = right.at[0, t, a]
            def sent(s):
                to(r, r, s, s, {"x": xp}).wait_send()
            @pl.when(zd[par] < NZ - 1)
            def _():
                sent(zs.at[t, a])
            sent(xs.at[t, a, 0])
            sent(xs.at[t, a, 1])
            sent(rs.at[t, a, 0])
        return carry
    lax.fori_loop(0, 4 * NA, drain, 0)

def comm(pay):
    V = pl.BlockSpec(memory_space=pltpu.VMEM)
    D = pltpu.SemaphoreType.DMA
    return pl.pallas_call(
        comm_kernel,
        out_shape=[jax.ShapeDtypeStruct(s, F32) for s in ((NTC, NA, PR, 128), (NX, NTC, NA, PR, 128), (NTC, NTC, PR, 128))],
        in_specs=[V], out_specs=[V] * 3,
        scratch_shapes=[D((8, 3)), D((8,)), D((8, 5)), D((8, 5, 2)), D((8, 5, 1)), D((4, 8, 5)), D((8, 3)), D((8,))],
        compiler_params=pltpu.CompilerParams(collective_id=0, has_side_effects=True, vmem_limit_bytes=60 * 2**20),
    )(pay)

def tile_of(lead, i, t):
    return lead[i, t, 8:, :]

def symmetric(tile):
    row = lax.broadcasted_iota(jnp.int32, tile.shape, 0)
    lane = lax.broadcasted_iota(jnp.int32, tile.shape, 1)
    return jnp.where(row >= lane, tile, tile.T)

def fill_symmetric(a_ref, tile):
    for i in range(PT):
        for t in range(i + 1):
            here = slice(i * 128, (i + 1) * 128), slice(t * 128, (t + 1) * 128)
            value = tile(i, t)
            if i == t:
                a_ref[here] = symmetric(value)
            else:
                a_ref[here] = value
                a_ref[here[1], here[0]] = value.T

def chain_kernel(pos, lead, w0h, w0l, p0h, p0l, w1h, w1l, edge, a, u, w, t):
    z, q = pos[0], pos[1]

    def edge_tile(first):
        @pl.when((z >= first) & (z < first + PT) & (q >= first) & (q <= z))
        def _():
            rows = pl.ds(pl.multiple_of((q - first) * 128, 128), 128)
            lanes = pl.ds(pl.multiple_of((z - first) * 128, 128), 128)
            edge[...] = u[rows, lanes].T

    edge[...] = jnp.zeros_like(edge)
    fill_symmetric(a, lambda i, k: tile_of(lead, i, k))
    factor_block(a, u, w, t)
    edge_tile(0)
    w0h[...], w0l[...] = halves(w[...])
    for i in range(PT):
        rows = slice(i * 128, (i + 1) * 128)
        raw = jnp.concatenate([tile_of(lead, PT + i, k) for k in range(PT)], axis=1)
        p0h[rows], p0l[rows] = halves(mm3(halves(raw), (w0h[...], w0l[...]), NT))

    def updated(i, k):
        hi = slice(i * 128, (i + 1) * 128), slice(k * 128, (k + 1) * 128)
        coarse = mm(p0h[hi[0]], p0h[hi[1]], NT)
        extra = mm(p0h[hi[0]], p0l[hi[1]], NT) + mm(p0l[hi[0]], p0h[hi[1]], NT)
        marked = lead[PT + i, PT + k, 0:1, :] > 0.5
        return tile_of(lead, PT + i, PT + k) - coarse - jnp.where(marked, 0.0, extra)

    fill_symmetric(a, updated)
    factor_block(a, u, w, t)
    edge_tile(PT)
    w1h[...], w1l[...] = halves(w[...])

def chain(pos, lead):
    wide = PT * 128
    V = pl.BlockSpec(memory_space=pltpu.VMEM)
    half = jax.ShapeDtypeStruct((wide, wide), BF16)
    return pl.pallas_call(
        chain_kernel,
        out_shape=[half] * 6 + [jax.ShapeDtypeStruct((128, 128), F32)],
        in_specs=[pl.BlockSpec(memory_space=pltpu.SMEM), V],
        out_specs=[V] * 7,
        scratch_shapes=[pltpu.VMEM((wide, wide), F32)] * 3 + [pltpu.VMEM((128, 2 * wide), F32)],
        compiler_params=pltpu.CompilerParams(vmem_limit_bytes=60 * 2**20),
    )(pos, lead)

def finish_kernel(pos, marks, left, right, w0h, w0l, p0h, p0l, w1h, w1l, edge, work, out, lh, ll, rh, rl):
    r, q = pos[2], pos[1]
    group = pl.program_id(0)
    wide = PT * 128

    def solve(read, count, high, low):
        raw = jnp.concatenate(
            [jnp.concatenate([read(m, k)[8:] for k in range(PT)], axis=1) for m in range(count)], axis=0)
        first = halves(mm3(halves(raw), (w0h[...], w0l[...]), NT))
        high[:, :wide], low[:, :wide] = first
        coarse = mm(first[0], p0h[...], NT)
        extra = mm(first[0], p0l[...], NT) + mm(first[1], p0h[...], NT)
        parts = []
        for m in range(count):
            rows = slice(m * 128, (m + 1) * 128)
            row = []
            for k in range(PT):
                lanes = slice(k * 128, (k + 1) * 128)
                piece = read(m, PT + k)
                row.append(piece[8:] - coarse[rows, lanes] - jnp.where(piece[0:1] > 0.5, 0.0, extra[rows, lanes]))
            parts.append(jnp.concatenate(row, axis=1))
        second = halves(mm3(halves(jnp.concatenate(parts, axis=0)), (w1h[...], w1l[...]), NT))
        high[:, wide:], low[:, wide:] = second

    @pl.when(group == 0)
    def _():
        solve(lambda m, k: left[k, m], NA, lh, ll)

    solve(lambda m, k: right[m, k, 0], NX, rh, rl)

    def one_row(a, carry):
        i = a * 32 + r

        @pl.when(a >= group)
        def _():
            rows = pl.ds(pl.multiple_of(a * 128, 128), 128)
            own_h, own_l = lh[rows, :], ll[rows, :]
            coarse = mm(own_h, rh[...], NT)
            extra = mm(own_h, rl[...], NT) + mm(own_l, rh[...], NT)
            for m in range(NX):
                lanes = slice(m * 128, (m + 1) * 128)
                j = group * 32 + m * 8 + q
                mark = marks[a, group * NX + m]
                tile = work[a, m]
                exact = tile - (coarse[:, lanes] + extra[:, lanes])
                rough = tile.astype(BF16).astype(F32) - coarse[:, lanes]
                rough = rough.astype(BF16).astype(F32)
                value = jnp.where(mark == 1, rough, exact)
                out[a, m] = jnp.where(i >= j, value, 0.0)

        @pl.when(a < group)
        def _():
            out[a] = jnp.zeros((NX, 128, 128), F32)
        return carry

    lax.fori_loop(0, NA, one_row, 0)

    @pl.when(group == 0)
    def _():
        lanes = pl.ds(pl.multiple_of(q * 128, 128), 128)
        for a in range(NA):
            i = a * 32 + r
            rows = slice(a * 128, (a + 1) * 128)
            value = lh[rows, lanes].astype(F32) + ll[rows, lanes].astype(F32)
            if a == 0:
                value = jnp.where((i < 2 * PT) & (i // PT == q // PT), edge[...], value)
            value = jnp.where(marks[a, 0] == 1, value.astype(BF16).astype(F32), value)
            out[a, 0] = jnp.where(i >= q, value, 0.0)

def finish(pos, marks, left, right, parts, work):
    wide = PT * 128
    S = pl.BlockSpec(memory_space=pltpu.SMEM)
    whole = lambda s: pl.BlockSpec(s, lambda g: (0,) * len(s))
    tiles = pl.BlockSpec((NA, NX, 128, 128), lambda g: (0, g, 0, 0))
    return pl.pallas_call(
        finish_kernel,
        grid=(NA,),
        out_shape=jax.ShapeDtypeStruct(work.shape, F32),
        in_specs=[S, S, whole(left.shape), pl.BlockSpec((NX, NTC, 1, PR, 128), lambda g: (0, 0, g, 0, 0))]
        + [whole(v.shape) for v in parts] + [tiles],
        out_specs=tiles,
        scratch_shapes=[pltpu.VMEM((NA * 128, 2 * wide), BF16)] * 2 + [pltpu.VMEM((NX * 128, 2 * wide), BF16)] * 2,
        compiler_params=pltpu.CompilerParams(vmem_limit_bytes=60 * 2**20, dimension_semantics=("arbitrary",)),
    )(pos, marks, left, right, *parts, work)

def on_device(matrix, flags):
    x, z, y, c = (lax.axis_index(n) for n in ("x", "z", "y", "c"))
    tiles = matrix.reshape(NA, NA * NX, 128, 128)
    marks = flags.reshape(NA, NA * NX)
    first = marks[:, 0][:, None, None]
    own = tiles[:, 0]
    own = jnp.where(first == 1, lax.reduce_precision(own, 8, 7), own)
    pay = jnp.concatenate([jnp.broadcast_to(first.astype(F32), (NA, 8, 128)), own], axis=1)
    left, right, lead = comm(pay)
    pos = jnp.stack([jnp.where(x == 0, z, 4 * PT), 2 * y + c, 8 * x + z]).astype(jnp.int32)
    parts = chain(pos, lead)
    return finish(pos, marks, left, right, parts, tiles).reshape(matrix.shape)

def solution(mesh):
    finer = Mesh(mesh.devices.reshape(NX, NZ, NY, 2), ("x", "z", "y", "c"))
    rows, cols = ("x", "z"), ("y", "c")
    return jax.shard_map(
        on_device, mesh=finer, in_specs=(P(None, rows, None, cols, None, None), P(None, rows, None, cols)),
        out_specs=P(None, rows, None, cols, None, None), check_vma=False)
```

```python
import jax
import jax.numpy as jnp
from jax import lax
from jax.experimental import pallas as pl
from jax.experimental.pallas import tpu as pltpu
from jax.sharding import Mesh
from jax.sharding import PartitionSpec as P

F32 = jnp.float32
BF16 = jnp.bfloat16
MESH = pl.DeviceIdType.MESH
PT = 4
HI = lax.Precision.HIGHEST
SUB = 32

def halves(v):
    high = v.astype(BF16)
    return high, (v - high.astype(F32)).astype(BF16)

NT = (((1,), (1,)), ((), ()))
TN = (((0,), (0,)), ((), ()))
NN = (((1,), (0,)), ((), ()))

def mm(a, b, dims):
    return lax.dot_general(a, b, dims, preferred_element_type=F32)

def mm6(a, b, dims):
    return lax.dot_general(a, b, dims, precision=HI, preferred_element_type=F32)

def mm3(a, b, dims):
    return mm(a[0], b[0], dims) + (mm(a[0], b[1], dims) + mm(a[1], b[0], dims))

def small_inverse(block):
    lanes = block.shape[1]
    groups = []
    for g in range(SUB // 8):
        low = 8 * g
        groups.append([jnp.broadcast_to(block[low:, low + e:low + e + 1], (SUB - low, lanes)) for e in range(8)])
    row = lax.broadcasted_iota(jnp.int32, (SUB, lanes), 0)
    lane = lax.broadcasted_iota(jnp.int32, (SUB, lanes), 1)
    right = (row == lane).astype(F32)
    done = []
    cols = [jnp.stack(g, axis=0) for g in groups]
    for g in range(SUB // 8):
        for e in range(8):
            own = cols[g][0]
            scale = lax.rsqrt(own[e:e + 1])
            factor = own * scale
            solved = right[e:e + 1] * scale
            done.append(solved)
            right = right - factor * solved
            if e < 7:
                cols[g] = cols[g][1:] - factor[None] * factor[e + 1:8][:, None]
            for h in range(g + 1, SUB // 8):
                off = 8 * (h - g)
                cols[h] = cols[h] - factor[off:][None] * factor[off:off + 8][:, None]
        right = right[8:]
    return jnp.concatenate(done, axis=0)

def factor_unit(kb, s, a_ref, u_ref, w_ref, t_ref):
    n = a_ref.shape[0]
    here = pl.ds(pl.multiple_of(kb * 128, 128), 128)

    @pl.when(s == 0)
    def _():
        row = lax.broadcasted_iota(jnp.int32, (128, n), 0)
        lane = lax.broadcasted_iota(jnp.int32, (128, n), 1)
        t_ref[:, :n] = a_ref[here, :]
        t_ref[:, n:] = (lane == row + kb * 128).astype(F32)

        @pl.when(kb > 0)
        def _():
            left = u_ref[:, here]
            t_ref[:, :n] -= mm6(left, u_ref[...], TN)
            t_ref[:, n:] -= mm6(left, w_ref[...], TN)

    rows = pl.ds(pl.multiple_of(s * SUB, SUB), SUB)
    out = pl.ds(pl.multiple_of(kb * 128 + s * SUB, SUB), SUB)
    inv = small_inverse(pltpu.roll(t_ref[rows, here], (128 - s * SUB) % 128, 1))[:, :SUB]
    both = mm6(inv, t_ref[rows, :], NN)
    lane = lax.broadcasted_iota(jnp.int32, (SUB, n), 1)
    row = lax.broadcasted_iota(jnp.int32, (SUB, n), 0) + (kb * 128 + s * SUB)
    u_ref[out, :] = jnp.where(lane >= row, both[:, :n], 0.0)
    w_ref[out, :] = jnp.where(lane <= row, both[:, n:], 0.0)
    left = u_ref[out, here]
    t_ref[...] -= mm6(left, both, TN)

def tile_of(lead, i, t):
    return lead[t, i, 8:, :]

def symmetric(tile):
    row = lax.broadcasted_iota(jnp.int32, tile.shape, 0)
    lane = lax.broadcasted_iota(jnp.int32, tile.shape, 1)
    return jnp.where(row >= lane, tile, tile.T)

def fill_symmetric(a_ref, tile):
    for i in range(PT):
        for t in range(i + 1):
            here = slice(i * 128, (i + 1) * 128), slice(t * 128, (t + 1) * 128)
            value = tile(i, t)
            if i == t:
                a_ref[here] = symmetric(value)
            else:
                a_ref[here] = value
                a_ref[here[1], here[0]] = value.T

def edge_tile(z, q, first, edge, u):
    @pl.when((z >= first) & (z < first + PT) & (q >= first) & (q <= z))
    def _():
        rows = pl.ds(pl.multiple_of(lax.rem(q, PT) * 128, 128), 128)
        lanes = pl.ds(pl.multiple_of(lax.rem(z, PT) * 128, 128), 128)
        edge[...] = u[rows, lanes].T

def chain_open(lead, edge, a, u, w):
    edge[...] = jnp.zeros_like(edge)
    fill_symmetric(a, lambda i, k: tile_of(lead, i, k))
    u[...] = jnp.zeros_like(u)
    w[...] = jnp.zeros_like(w)

def chain_turn(z, q, lead, w0h, w0l, p0h, p0l, edge, a, u, w):
    edge_tile(z, q, 0, edge, u)
    w0h[...], w0l[...] = halves(w[...])
    for i in range(PT):
        rows = slice(i * 128, (i + 1) * 128)
        raw = jnp.concatenate([tile_of(lead, PT + i, k) for k in range(PT)], axis=1)
        p0h[rows], p0l[rows] = halves(mm3(halves(raw), (w0h[...], w0l[...]), NT))

    def updated(i, k):
        hi = slice(i * 128, (i + 1) * 128), slice(k * 128, (k + 1) * 128)
        coarse = mm(p0h[hi[0]], p0h[hi[1]], NT)
        extra = mm(p0h[hi[0]], p0l[hi[1]], NT) + mm(p0l[hi[0]], p0h[hi[1]], NT)
        marked = lead[PT + k, PT + i, 0:1, :] > 0.5
        return tile_of(lead, PT + i, PT + k) - coarse - jnp.where(marked, 0.0, extra)

    fill_symmetric(a, updated)
    u[...] = jnp.zeros_like(u)
    w[...] = jnp.zeros_like(w)

def chain_close(z, q, w1h, w1l, edge, u, w):
    edge_tile(z, q, PT, edge, u)
    w1h[...], w1l[...] = halves(w[...])

UNITS = 2 * PT * 128 // SUB

def chain_unit(n, z, q, lead, outs, edge, a, u, w, t):
    half = UNITS // 2

    @pl.when(n == half)
    def _():
        chain_turn(z, q, lead, *outs[:4], edge, a, u, w)
    k = lax.rem(n, half)
    factor_unit(k // (128 // SUB), lax.rem(k, 128 // SUB), a, u, w, t)

NX, NZ, NY, NA, NTC = 4, 8, 4, 5, 8
PR = 136
ZL, RL, FL, OFF = 1, 2, 4, 1
NS = 3
OPEN = 3
PER = 2

def move_kernel(with_chain, pay_ref, left, right, lead, w0h, w0l, p0h, p0l, w1h, w1l, edge,
                a_ref, u_ref, w_ref, t_ref, ls, lr, zs, xs, rs, rr, qs, qr, gs, gr, hs, hr):
    x, z, y, c = (lax.axis_index(n) for n in ("x", "z", "y", "c"))
    q = 2 * y + c
    xp, xm, xfar = lax.rem(x + 1, NX), lax.rem(x + NX - 1, NX), lax.rem(x + 2, NX)
    zp, zm = lax.rem(z + 1, NZ), lax.rem(z + NZ - 1, NZ)
    yp, ym, yo = lax.rem(y + 1, NY), lax.rem(y + NY - 1, NY), lax.rem(y + 2, NY)
    other = {"c": 1 - c}

    def to(src, dst, send, recv, where):
        return pltpu.make_async_remote_copy(src_ref=src, dst_ref=dst, send_sem=send, recv_sem=recv,
                                            device_id=where, device_id_type=MESH)

    barrier = pltpu.get_barrier_semaphore()
    peers = [{"x": xp}, {"x": xm}, {"z": zp}, {"z": zm}, {"y": yp}, {"y": ym}, other]
    for p in peers:
        pl.semaphore_signal(barrier, inc=1, device_id=p, device_id_type=MESH)
    pl.semaphore_wait(barrier, len(peers))

    class Gather:
        def __init__(self, own, slot, send, recv, limit):
            self.own, self.slot, self.send, self.recv, self.limit = own, slot, send, recv, limit

        def on(self, k, fn):
            if self.limit == NTC:
                fn()
            else:
                pl.when(k < self.limit)(fn)

        def copy(self, src, k, i, where):
            return to(src, self.slot(k), self.send.at[k, i], self.recv.at[k], where)

        def got(self, k):
            self.copy(self.slot(k), k, 0, other).wait_recv()

        def open(self):
            def go():
                for i, where in enumerate(({"y": yp}, {"y": ym}, other)):
                    self.copy(self.own, q, i, where).start()
            self.on(q, go)

        def pass_on(self):
            for k, core, where in ((2 * ym + c, 0, {"y": yp}), (2 * yp + c, 1, {"y": ym})):
                def go(k=k, core=core, where=where):
                    self.got(k)
                    @pl.when(c == core)
                    def _():
                        self.copy(self.slot(k), k, 0, where).start()
                    self.copy(self.slot(k), k, 2, other).start()
                self.on(k, go)

        def share(self):
            k = 2 * yo + c
            def go():
                self.got(k)
                self.copy(self.slot(k), k, 2, other).start()
            self.on(k, go)

        def close(self):
            for n in range(NY):
                k = 2 * n + 1 - c
                self.on(k, lambda k=k: self.got(k))

        def drain(self):
            def sent(k, i):
                self.copy(self.slot(k), k, i, other).wait_send()
            self.on(q, lambda: [sent(q, i) for i in range(3)] and None)
            for k, core in ((2 * ym + c, 0), (2 * yp + c, 1)):
                def go(k=k, core=core):
                    pl.when(c == core)(lambda: sent(k, 0))
                    sent(k, 2)
                self.on(k, go)
            self.on(2 * yo + c, lambda: sent(2 * yo + c, 2))

    sides = Gather(pay_ref, lambda k: left.at[k], ls, lr, NTC)
    upper = Gather(lead.at[q, pl.ds(0, PT)], lambda k: lead.at[k, pl.ds(0, PT)], gs, gr, PT)
    lower = Gather(lead.at[q, pl.ds(PT, PT)], lambda k: lead.at[k, pl.ds(PT, PT)], hs, hr, NTC)

    sides.open()

    mine = pay_ref.at[0]
    def tip(row, send, where, src=None):
        slot = lead.at[q, row]
        return to(slot if src is None else src, slot, qs.at[send], qr.at[row], where)

    @pl.when(x == 0)
    def _():
        tip(z, 0, {"x": xp}, mine).start()
        tip(z, 1, {"x": xm}, mine).start()
        lead[pl.ds(q, 1), pl.ds(z, 1)] = pay_ref[0][None, None]
        tip(z, 2, {"z": zp}, mine).start()
        tip(z, 6, {"z": zm}, mine).start()

    @pl.when(x > 0)
    def _():
        tip(z, 0, other).wait_recv()
        @pl.when(x == 1)
        def _():
            tip(z, 0, {"x": xp}).start()
        tip(z, 2, {"z": zp}).start()
        tip(z, 6, {"z": zm}).start()

    for h in range(1, 5):
        row = lax.rem(z - h + NZ, NZ)
        tip(row, 0, other).wait_recv()
        if h < 4:
            tip(row, 2 + h, {"z": zp}).start()
            row = lax.rem(z + h, NZ)
            tip(row, 0, other).wait_recv()
            if h < 3:
                tip(row, 6 + h, {"z": zm}).start()

    upper.open()
    sides.pass_on()
    lower.open()
    sides.share()
    sides.close()
    left[pl.ds(q, 1)] = pay_ref[...][None]

    zd = (lax.rem(z - q + NZ, NZ), lax.rem(q - z + NZ, NZ))
    znext = ({"z": zp}, {"z": zm})
    xnext = ({"x": xp}, {"x": xm})
    xprev = (xm, xp)

    def landed(src, t, a):
        r = right.at[src, t, a]
        to(r, r, rs.at[t, a], rr.at[src, t, a], other).wait_recv()

    def push(src, t, a, send, where, ref=None):
        r = right.at[src, t, a]
        to(r if ref is None else ref, r, send, rr.at[src, t, a], where).start()

    def inside(n, low, high, fn):
        pl.when((n >= low) & (n < high))(fn)

    def near(par, n):
        t, a = 2 * lax.rem(n, 4) + par, n // 4

        def send(ref):
            @pl.when(zd[par] < NZ - 1)
            def _():
                push(x, t, a, zs.at[x, t, a], znext[par], ref)
            push(x, t, a, xs.at[t, a, 0], {"x": xp}, ref)
            push(x, t, a, xs.at[t, a, 1], {"x": xm}, ref)

        @pl.when(zd[par] == 0)
        def _():
            send(left.at[t, a])

        @pl.when(zd[par] > 0)
        def _():
            landed(x, t, a)
            send(None)

    def relay(par, n):
        t, a = 2 * lax.rem(n, 4) + par, n // 4
        landed(xprev[par], t, a)
        push(xprev[par], t, a, rs.at[t, a], xnext[par])

    def last_landed(par, n):
        t, a = 2 * lax.rem(n, 4) + par, n // 4
        landed(xprev[1 - par], t, a)
        landed(xfar, t, a)

    def spread(par, n):
        t, a = 2 * lax.rem(n, 4) + par, n // 4
        push(x, t, a, xs.at[t, a, 0], {"x": xp}, left.at[t, a])
        push(x, t, a, xs.at[t, a, 1], {"x": xm}, left.at[t, a])

    far = 4 * (NA - NS)

    def stream(par, k):
        rel, j = k // far, lax.rem(k, far)
        t, a = 2 * lax.rem(j, 4) + par, NS + j // 4
        sign = 3 if par == 0 else 1
        src = lax.rem(x + jnp.where(rel == 0, 0, jnp.where(rel == 1, sign, jnp.where(rel == 2, 4 - sign, 2))), NX)

        @pl.when((zd[par] > 0) | (rel > 1))
        def _():
            landed(src, t, a)

        @pl.when(zd[par] < NZ - 1)
        def _():
            own = (zd[par] == 0) & (rel == 0)
            @pl.when(own)
            def _():
                push(src, t, a, zs.at[src, t, a], znext[par], left.at[t, a])

            @pl.when(jnp.logical_not(own))
            def _():
                push(src, t, a, zs.at[src, t, a], znext[par])

    def step(m, carry):
        for par in range(2):
            n = m - zd[par] * ZL
            inside(n, 0, 4 * NS, lambda: near(par, n))
            @pl.when((zd[par] == 0) & (n < far // 2))
            def _():
                spread(par, 4 * NS + 2 * n)
                spread(par, 4 * NS + 2 * n + 1)
            inside(n - RL, 0, 4 * NS, lambda: relay(par, n - RL))
            @pl.when((zd[par] == 0) & (n >= RL) & (n < far // 2 + RL))
            def _():
                relay(par, 4 * NS + 2 * (n - RL))
                relay(par, 4 * NS + 2 * (n - RL) + 1)
            for i in range(3):
                k = 3 * (n - OFF) + i
                inside(k, 0, NX * far, lambda: stream(par, k))
            inside(n - FL, 0, 4 * NS, lambda: last_landed(par, n - FL))
        pl.when(m == 1)(upper.pass_on)
        @pl.when(m == OPEN)
        def _():
            upper.share()
            upper.close()
            chain_open(lead, edge, a_ref, u_ref, w_ref)
        pl.when(m == OPEN + 1)(lower.pass_on)
        pl.when(m == OPEN + 3)(lower.share)
        pl.when(m == OPEN + 5)(lower.close)
        for i in range(PER):
            unit = PER * (m - OPEN) + i
            inside(unit, 0, UNITS, lambda: chain_unit(
                unit, jnp.where(x == 0, z, 4 * PT), q, lead, (w0h, w0l, p0h, p0l), edge, a_ref, u_ref, w_ref, t_ref))
        return carry

    steps = max(4 * NS + 7 * ZL + FL, OPEN + UNITS // PER)
    lax.fori_loop(0, steps, step, 0)
    chain_close(jnp.where(x == 0, z, 4 * PT), q, w1h, w1l, edge, u_ref, w_ref)

    @pl.when(z == q)
    def _():
        right[pl.ds(x, 1)] = left[...][None]

    sides.drain()
    upper.drain()
    lower.drain()

    def tip_sent(i):
        tip(z, i, other).wait_send()

    pl.when(x <= 1)(lambda: tip_sent(0))
    pl.when(x == 0)(lambda: tip_sent(1))
    for i in range(2, 9):
        tip_sent(i)

    def drain(n, carry):
        for par in range(2):
            t, a = 2 * lax.rem(n, 4) + par, n // 4
            def sent(s):
                r = right.at[0, t, a]
                to(r, r, s, s, other).wait_send()

            @pl.when((n < 4 * NS) | (zd[par] == 0))
            def _():
                sent(xs.at[t, a, 0])
                sent(xs.at[t, a, 1])
                sent(rs.at[t, a])

            @pl.when(zd[par] < NZ - 1)
            def _():
                @pl.when(n < 4 * NS)
                def _():
                    sent(zs.at[x, t, a])

                @pl.when(n >= 4 * NS)
                def _():
                    for k in range(NX):
                        sent(zs.at[k, t, a])
        return carry
    lax.fori_loop(0, 4 * NA, drain, 0)

def move(pay):
    V = pl.BlockSpec(memory_space=pltpu.VMEM)
    D = pltpu.SemaphoreType.DMA
    wide = PT * 128
    half = jax.ShapeDtypeStruct((wide, wide), BF16)
    shape = lambda *s: jax.ShapeDtypeStruct(s, F32)
    return pl.pallas_call(
        lambda *r: move_kernel(True, *r[:3], r[10], *r[3:10], *r[11:]),
        out_shape=[shape(NTC, NA, PR, 128), shape(NX, NTC, NA, PR, 128)] + [half] * 6 + [shape(128, 128)],
        in_specs=[V], out_specs=[V] * 9,
        scratch_shapes=[pltpu.VMEM((NTC, NTC, PR, 128), F32)] + [pltpu.VMEM((wide, wide), F32)] * 3
        + [pltpu.VMEM((128, 2 * wide), F32)]
        + [D((8, 3)), D((8,)), D((4, 8, 5)), D((8, 5, 2)), D((8, 5)), D((4, 8, 5)), D((9,)), D((8,)),
           D((8, 3)), D((8,)), D((8, 3)), D((8,))],
        compiler_params=pltpu.CompilerParams(collective_id=0, has_side_effects=True, vmem_limit_bytes=60 * 2**20),
    )(pay)

def finish_kernel(pos, marks, left, right, w0h, w0l, p0h, p0l, w1h, w1l, edge, work, out, lh, ll, rh, rl):
    r, q = pos[2], pos[1]
    group = pl.program_id(0)
    wide = PT * 128

    def solve(read, count, high, low):
        raw = jnp.concatenate(
            [jnp.concatenate([read(m, k)[8:] for k in range(PT)], axis=1) for m in range(count)], axis=0)
        first = halves(mm3(halves(raw), (w0h[...], w0l[...]), NT))
        high[:, :wide], low[:, :wide] = first
        coarse = mm(first[0], p0h[...], NT)
        extra = mm(first[0], p0l[...], NT) + mm(first[1], p0h[...], NT)
        parts = []
        for m in range(count):
            rows = slice(m * 128, (m + 1) * 128)
            row = []
            for k in range(PT):
                lanes = slice(k * 128, (k + 1) * 128)
                piece = read(m, PT + k)
                row.append(piece[8:] - coarse[rows, lanes] - jnp.where(piece[0:1] > 0.5, 0.0, extra[rows, lanes]))
            parts.append(jnp.concatenate(row, axis=1))
        second = halves(mm3(halves(jnp.concatenate(parts, axis=0)), (w1h[...], w1l[...]), NT))
        high[:, wide:], low[:, wide:] = second

    @pl.when(group == 0)
    def _():
        solve(lambda m, k: left[k, m], NA, lh, ll)

    solve(lambda m, k: right[m, k, 0], NX, rh, rl)

    def one_row(a, carry):
        i = a * 32 + r

        @pl.when(a >= group)
        def _():
            rows = pl.ds(pl.multiple_of(a * 128, 128), 128)
            own_h, own_l = lh[rows, :], ll[rows, :]
            coarse = mm(own_h, rh[...], NT)
            extra = mm(own_h, rl[...], NT) + mm(own_l, rh[...], NT)
            for m in range(NX):
                lanes = slice(m * 128, (m + 1) * 128)
                j = group * 32 + m * 8 + q
                mark = marks[a, group * NX + m]
                tile = work[a, m]
                exact = tile - (coarse[:, lanes] + extra[:, lanes])
                rough = tile.astype(BF16).astype(F32) - coarse[:, lanes]
                rough = rough.astype(BF16).astype(F32)
                value = jnp.where(mark == 1, rough, exact)
                out[a, m] = jnp.where(i >= j, value, 0.0)

        @pl.when(a < group)
        def _():
            out[a] = jnp.zeros((NX, 128, 128), F32)
        return carry

    lax.fori_loop(0, NA, one_row, 0)

    @pl.when(group == 0)
    def _():
        lanes = pl.ds(pl.multiple_of(q * 128, 128), 128)
        for a in range(NA):
            i = a * 32 + r
            rows = slice(a * 128, (a + 1) * 128)
            value = lh[rows, lanes].astype(F32) + ll[rows, lanes].astype(F32)
            if a == 0:
                value = jnp.where((i < 2 * PT) & (i // PT == q // PT), edge[...], value)
            value = jnp.where(marks[a, 0] == 1, value.astype(BF16).astype(F32), value)
            out[a, 0] = jnp.where(i >= q, value, 0.0)

def finish(pos, marks, left, right, parts, work):
    wide = PT * 128
    S = pl.BlockSpec(memory_space=pltpu.SMEM)
    whole = lambda s: pl.BlockSpec(s, lambda g: (0,) * len(s))
    tiles = pl.BlockSpec((NA, NX, 128, 128), lambda g: (0, g, 0, 0))
    return pl.pallas_call(
        finish_kernel,
        grid=(NA,),
        out_shape=jax.ShapeDtypeStruct(work.shape, F32),
        in_specs=[S, S, whole(left.shape), pl.BlockSpec((NX, NTC, 1, PR, 128), lambda g: (0, 0, g, 0, 0))]
        + [whole(v.shape) for v in parts] + [tiles],
        out_specs=tiles,
        scratch_shapes=[pltpu.VMEM((NA * 128, 2 * wide), BF16)] * 2 + [pltpu.VMEM((NX * 128, 2 * wide), BF16)] * 2,
        compiler_params=pltpu.CompilerParams(vmem_limit_bytes=60 * 2**20, dimension_semantics=("arbitrary",)),
    )(pos, marks, left, right, *parts, work)

def on_device(matrix, flags):
    x, z, y, c = (lax.axis_index(n) for n in ("x", "z", "y", "c"))
    tiles = matrix.reshape(NA, NA * NX, 128, 128)
    marks = flags.reshape(NA, NA * NX)
    first = marks[:, 0][:, None, None]
    own = tiles[:, 0]
    own = jnp.where(first == 1, lax.reduce_precision(own, 8, 7), own)
    pay = jnp.concatenate([jnp.broadcast_to(first.astype(F32), (NA, 8, 128)), own], axis=1)
    left, right, *parts = move(pay)
    pos = jnp.stack([jnp.where(x == 0, z, 4 * PT), 2 * y + c, 8 * x + z]).astype(jnp.int32)
    return finish(pos, marks, left, right, parts, tiles).reshape(matrix.shape)

def solution(mesh):
    finer = Mesh(mesh.devices.reshape(NX, NZ, NY, 2), ("x", "z", "y", "c"))
    rows, cols = ("x", "z"), ("y", "c")
    return jax.shard_map(
        on_device, mesh=finer, in_specs=(P(None, rows, None, cols, None, None), P(None, rows, None, cols)),
        out_specs=P(None, rows, None, cols, None, None), check_vma=False)
```

```python
import jax
import jax.numpy as jnp
from jax import lax
from jax.experimental import pallas as pl
from jax.experimental.pallas import tpu as pltpu
from jax.sharding import Mesh
from jax.sharding import PartitionSpec as P

F32 = jnp.float32
BF16 = jnp.bfloat16
MESH = pl.DeviceIdType.MESH
PT = 4
HI = lax.Precision.HIGHEST
SUB = 32

def halves(v):
    high = v.astype(BF16)
    return high, (v - high.astype(F32)).astype(BF16)

NT = (((1,), (1,)), ((), ()))
TN = (((0,), (0,)), ((), ()))
NN = (((1,), (0,)), ((), ()))

def mm(a, b, dims):
    return lax.dot_general(a, b, dims, preferred_element_type=F32)

def mm6(a, b, dims):
    return lax.dot_general(a, b, dims, precision=HI, preferred_element_type=F32)

def mm3(a, b, dims):
    return mm(a[0], b[0], dims) + (mm(a[0], b[1], dims) + mm(a[1], b[0], dims))

HALF = PT * 128 // 2

def triple(v, axis):
    h, l = halves(v)
    return jnp.concatenate([h, h, l], axis=axis)

def keep_factor(w, wa, wb):
    h, l = halves(w)
    wa[...] = jnp.concatenate([h[:HALF, :HALF], l[:HALF, :HALF], h[:HALF, :HALF]], axis=1)
    wb[...] = jnp.concatenate([h[HALF:], l[HALF:], h[HALF:]], axis=1)

def solve_rows(raw, wa, wb):
    top = mm(triple(raw[:, :HALF], 1), wa[...], NT)
    return jnp.concatenate([top, mm(triple(raw, 1), wb[...], NT)], axis=1)

def small_inverse(block):
    lanes = block.shape[1]
    cols = []
    for k in range(SUB):
        low = 8 * (k // 8)
        cols.append(jnp.broadcast_to(block[low:, k:k + 1], (SUB - low, lanes)))
    row = lax.broadcasted_iota(jnp.int32, (SUB, lanes), 0)
    lane = lax.broadcasted_iota(jnp.int32, (SUB, lanes), 1)
    right = (row == lane).astype(F32)
    done = []
    for k in range(SUB):
        low = 8 * (k // 8)
        own = cols[k]
        scale = lax.rsqrt(own[k - low:k - low + 1, :])
        factor = own * scale
        solved = right[k - low:k - low + 1, :] * scale
        done.append(solved)
        if k == SUB - 1:
            break
        nxt = 8 * ((k + 1) // 8)
        for m in range(k + 1, SUB):
            base = 8 * (m // 8)
            cols[m] = cols[m] - factor[base - low:, :] * factor[m - low:m - low + 1, :]
        right = right[nxt - low:, :] - factor[nxt - low:, :] * solved
    return jnp.concatenate(done, axis=0)

def factor_unit(kb, s, a_ref, u_ref, w_ref, t_ref):
    n = a_ref.shape[0]
    here = pl.ds(pl.multiple_of(kb * 128, 128), 128)

    @pl.when(s == 0)
    def _():
        row = lax.broadcasted_iota(jnp.int32, (128, n), 0)
        lane = lax.broadcasted_iota(jnp.int32, (128, n), 1)
        t_ref[:, :n] = a_ref[here, :]
        t_ref[:, n:] = (lane == row + kb * 128).astype(F32)

        @pl.when(kb > 0)
        def _():
            left = halves(u_ref[:, here])
            t_ref[:, :n] -= mm3(left, halves(u_ref[...]), TN)
            t_ref[:, n:] -= mm3(left, halves(w_ref[...]), TN)

    rows = pl.ds(pl.multiple_of(s * SUB, SUB), SUB)
    out = pl.ds(pl.multiple_of(kb * 128 + s * SUB, SUB), SUB)
    inv = small_inverse(pltpu.roll(t_ref[rows, here], (128 - s * SUB) % 128, 1))[:, :SUB]
    both = mm6(inv, t_ref[rows, :], NN)
    lane = lax.broadcasted_iota(jnp.int32, (SUB, n), 1)
    row = lax.broadcasted_iota(jnp.int32, (SUB, n), 0) + (kb * 128 + s * SUB)
    u_ref[out, :] = jnp.where(lane >= row, both[:, :n], 0.0)
    w_ref[out, :] = jnp.where(lane <= row, both[:, n:], 0.0)
    left = u_ref[out, here]
    hl, hb = halves(left), halves(both)
    t_ref[...] -= mm(jnp.concatenate([hl[0], hl[0], hl[1]], axis=0), jnp.concatenate([hb[0], hb[1], hb[0]], axis=0), TN)

def tile_of(lead, i, t):
    return lead[t, i, 8:, :]

def symmetric(tile):
    row = lax.broadcasted_iota(jnp.int32, tile.shape, 0)
    lane = lax.broadcasted_iota(jnp.int32, tile.shape, 1)
    return jnp.where(row >= lane, tile, tile.T)

def fill_symmetric(a_ref, tile):
    for i in range(PT):
        for t in range(i + 1):
            here = slice(i * 128, (i + 1) * 128), slice(t * 128, (t + 1) * 128)
            value = tile(i, t)
            if i == t:
                a_ref[here] = symmetric(value)
            else:
                a_ref[here] = value
                a_ref[here[1], here[0]] = value.T

def edge_tile(z, q, first, edge, u):
    @pl.when((z >= first) & (z < first + PT) & (q >= first) & (q <= z))
    def _():
        rows = pl.ds(pl.multiple_of(lax.rem(q, PT) * 128, 128), 128)
        lanes = pl.ds(pl.multiple_of(lax.rem(z, PT) * 128, 128), 128)
        edge[...] = u[rows, lanes].T

def chain_open(lead, edge, a, u, w):
    edge[...] = jnp.zeros_like(edge)
    fill_symmetric(a, lambda i, k: tile_of(lead, i, k))
    u[...] = jnp.zeros_like(u)
    w[...] = jnp.zeros_like(w)

def chain_turn(z, q, lead, w0a, w0b, p0h, p0x, edge, a, u, w):
    edge_tile(z, q, 0, edge, u)
    keep_factor(w[...], w0a, w0b)
    wide = PT * 128
    for i in range(PT):
        rows = slice(i * 128, (i + 1) * 128)
        raw = jnp.concatenate([tile_of(lead, PT + i, k) for k in range(PT)], axis=1)
        high, low = halves(solve_rows(raw, w0a, w0b))
        p0h[rows] = high
        p0x[rows, :wide], p0x[rows, wide:] = low, high

    def updated(i, k):
        hi = slice(i * 128, (i + 1) * 128), slice(k * 128, (k + 1) * 128)
        coarse = mm(p0h[hi[0]], p0h[hi[1]], NT)
        extra = mm(p0h[hi[0]], p0x[hi[1], :wide], NT) + mm(p0x[hi[0], :wide], p0h[hi[1]], NT)
        marked = lead[PT + k, PT + i, 0:1, :] > 0.5
        return tile_of(lead, PT + i, PT + k) - coarse - jnp.where(marked, 0.0, extra)

    fill_symmetric(a, updated)
    u[...] = jnp.zeros_like(u)
    w[...] = jnp.zeros_like(w)

def chain_close(z, q, w1a, w1b, edge, u, w):
    edge_tile(z, q, PT, edge, u)
    keep_factor(w[...], w1a, w1b)

UNITS = 2 * PT * 128 // SUB

def chain_unit(n, z, q, lead, outs, edge, a, u, w, t):
    half = UNITS // 2

    @pl.when(n == half)
    def _():
        chain_turn(z, q, lead, *outs[:4], edge, a, u, w)
    k = lax.rem(n, half)
    factor_unit(k // (128 // SUB), lax.rem(k, 128 // SUB), a, u, w, t)

NX, NZ, NY, NA, NTC = 4, 8, 4, 5, 8
PR = 136
ZL, RL, FL, OFF = 1, 2, 4, 1
NS = 3
OPEN = 3
PER = 2

def move_kernel(with_chain, pay_ref, left, right, lead, w0a, w0b, p0h, p0x, w1a, w1b, edge,
                a_ref, u_ref, w_ref, t_ref, ls, lr, zs, xs, rs, rr, qs, qr, gs, gr, hs, hr):
    x, z, y, c = (lax.axis_index(n) for n in ("x", "z", "y", "c"))
    q = 2 * y + c
    xp, xm, xfar = lax.rem(x + 1, NX), lax.rem(x + NX - 1, NX), lax.rem(x + 2, NX)
    zp, zm = lax.rem(z + 1, NZ), lax.rem(z + NZ - 1, NZ)
    yp, ym, yo = lax.rem(y + 1, NY), lax.rem(y + NY - 1, NY), lax.rem(y + 2, NY)
    other = {"c": 1 - c}

    def to(src, dst, send, recv, where):
        return pltpu.make_async_remote_copy(src_ref=src, dst_ref=dst, send_sem=send, recv_sem=recv,
                                            device_id=where, device_id_type=MESH)

    barrier = pltpu.get_barrier_semaphore()
    peers = [{"x": xp}, {"x": xm}, {"z": zp}, {"z": zm}, {"y": yp}, {"y": ym}, other]
    for p in peers:
        pl.semaphore_signal(barrier, inc=1, device_id=p, device_id_type=MESH)
    pl.semaphore_wait(barrier, len(peers))

    class Gather:
        def __init__(self, own, slot, send, recv, limit):
            self.own, self.slot, self.send, self.recv, self.limit = own, slot, send, recv, limit

        def on(self, k, fn):
            if self.limit == NTC:
                fn()
            else:
                pl.when(k < self.limit)(fn)

        def copy(self, src, k, i, where):
            return to(src, self.slot(k), self.send.at[k, i], self.recv.at[k], where)

        def got(self, k):
            self.copy(self.slot(k), k, 0, other).wait_recv()

        def open(self):
            def go():
                for i, where in enumerate(({"y": yp}, {"y": ym}, other)):
                    self.copy(self.own, q, i, where).start()
            self.on(q, go)

        def pass_on(self):
            for k, core, where in ((2 * ym + c, 0, {"y": yp}), (2 * yp + c, 1, {"y": ym})):
                def go(k=k, core=core, where=where):
                    self.got(k)
                    @pl.when(c == core)
                    def _():
                        self.copy(self.slot(k), k, 0, where).start()
                    self.copy(self.slot(k), k, 2, other).start()
                self.on(k, go)

        def share(self):
            k = 2 * yo + c
            def go():
                self.got(k)
                self.copy(self.slot(k), k, 2, other).start()
            self.on(k, go)

        def close(self):
            for n in range(NY):
                k = 2 * n + 1 - c
                self.on(k, lambda k=k: self.got(k))

        def drain(self):
            def sent(k, i):
                self.copy(self.slot(k), k, i, other).wait_send()
            self.on(q, lambda: [sent(q, i) for i in range(3)] and None)
            for k, core in ((2 * ym + c, 0), (2 * yp + c, 1)):
                def go(k=k, core=core):
                    pl.when(c == core)(lambda: sent(k, 0))
                    sent(k, 2)
                self.on(k, go)
            self.on(2 * yo + c, lambda: sent(2 * yo + c, 2))

    sides = Gather(pay_ref, lambda k: left.at[k], ls, lr, NTC)
    upper = Gather(lead.at[q, pl.ds(0, PT)], lambda k: lead.at[k, pl.ds(0, PT)], gs, gr, PT)
    lower = Gather(lead.at[q, pl.ds(PT, PT)], lambda k: lead.at[k, pl.ds(PT, PT)], hs, hr, NTC)

    sides.open()

    mine = pay_ref.at[0]
    def tip(row, send, where, src=None):
        slot = lead.at[q, row]
        return to(slot if src is None else src, slot, qs.at[send], qr.at[row], where)

    @pl.when(x == 0)
    def _():
        tip(z, 0, {"x": xp}, mine).start()
        tip(z, 1, {"x": xm}, mine).start()
        lead[pl.ds(q, 1), pl.ds(z, 1)] = pay_ref[0][None, None]
        tip(z, 2, {"z": zp}, mine).start()
        tip(z, 6, {"z": zm}, mine).start()

    @pl.when(x > 0)
    def _():
        tip(z, 0, other).wait_recv()
        @pl.when(x == 1)
        def _():
            tip(z, 0, {"x": xp}).start()
        tip(z, 2, {"z": zp}).start()
        tip(z, 6, {"z": zm}).start()

    for h in range(1, 5):
        if h == 2:
            sides.pass_on()
        if h == 4:
            sides.share()
        row = lax.rem(z - h + NZ, NZ)
        tip(row, 0, other).wait_recv()
        if h < 4:
            tip(row, 2 + h, {"z": zp}).start()
            row = lax.rem(z + h, NZ)
            tip(row, 0, other).wait_recv()
            if h < 3:
                tip(row, 6 + h, {"z": zm}).start()

    upper.open()
    lower.open()
    sides.close()
    left[pl.ds(q, 1)] = pay_ref[...][None]

    zd = (lax.rem(z - q + NZ, NZ), lax.rem(q - z + NZ, NZ))
    znext = ({"z": zp}, {"z": zm})
    xnext = ({"x": xp}, {"x": xm})
    xprev = (xm, xp)

    def landed(src, t, a):
        r = right.at[src, t, a]
        to(r, r, rs.at[t, a], rr.at[src, t, a], other).wait_recv()

    def push(src, t, a, send, where, ref=None):
        r = right.at[src, t, a]
        to(r if ref is None else ref, r, send, rr.at[src, t, a], where).start()

    def inside(n, low, high, fn):
        pl.when((n >= low) & (n < high))(fn)

    def near(par, n):
        t, a = 2 * lax.rem(n, 4) + par, n // 4

        def send(ref):
            @pl.when(zd[par] < NZ - 1)
            def _():
                push(x, t, a, zs.at[x, t, a], znext[par], ref)
            push(x, t, a, xs.at[t, a, 0], {"x": xp}, ref)
            push(x, t, a, xs.at[t, a, 1], {"x": xm}, ref)

        @pl.when(zd[par] == 0)
        def _():
            send(left.at[t, a])

        @pl.when(zd[par] > 0)
        def _():
            landed(x, t, a)
            send(None)

    def relay(par, n):
        t, a = 2 * lax.rem(n, 4) + par, n // 4
        landed(xprev[par], t, a)
        push(xprev[par], t, a, rs.at[t, a], xnext[par])

    def last_landed(par, n):
        t, a = 2 * lax.rem(n, 4) + par, n // 4
        landed(xprev[1 - par], t, a)
        landed(xfar, t, a)

    def spread(par, n):
        t, a = 2 * lax.rem(n, 4) + par, n // 4
        push(x, t, a, xs.at[t, a, 0], {"x": xp}, left.at[t, a])
        push(x, t, a, xs.at[t, a, 1], {"x": xm}, left.at[t, a])

    far = 4 * (NA - NS)

    def stream(par, k):
        rel, j = k // far, lax.rem(k, far)
        t, a = 2 * lax.rem(j, 4) + par, NS + j // 4
        sign = 3 if par == 0 else 1
        src = lax.rem(x + jnp.where(rel == 0, 0, jnp.where(rel == 1, sign, jnp.where(rel == 2, 4 - sign, 2))), NX)

        @pl.when((zd[par] > 0) | (rel > 1))
        def _():
            landed(src, t, a)

        @pl.when(zd[par] < NZ - 1)
        def _():
            own = (zd[par] == 0) & (rel == 0)
            @pl.when(own)
            def _():
                push(src, t, a, zs.at[src, t, a], znext[par], left.at[t, a])

            @pl.when(jnp.logical_not(own))
            def _():
                push(src, t, a, zs.at[src, t, a], znext[par])

    def step(m, carry):
        for par in range(2):
            n = m - zd[par] * ZL
            inside(n, 0, 4 * NS, lambda: near(par, n))
            @pl.when((zd[par] == 0) & (n < far // 2))
            def _():
                spread(par, 4 * NS + 2 * n)
                spread(par, 4 * NS + 2 * n + 1)
            inside(n - RL, 0, 4 * NS, lambda: relay(par, n - RL))
            @pl.when((zd[par] == 0) & (n >= RL) & (n < far // 2 + RL))
            def _():
                relay(par, 4 * NS + 2 * (n - RL))
                relay(par, 4 * NS + 2 * (n - RL) + 1)
            for i in range(3):
                k = 3 * (n - OFF) + i
                inside(k, 0, NX * far, lambda: stream(par, k))
            inside(n - FL, 0, 4 * NS, lambda: last_landed(par, n - FL))
        pl.when(m == 1)(upper.pass_on)
        @pl.when(m == OPEN)
        def _():
            upper.share()
            upper.close()
            chain_open(lead, edge, a_ref, u_ref, w_ref)
        pl.when(m == OPEN + 1)(lower.pass_on)
        pl.when(m == OPEN + 3)(lower.share)
        pl.when(m == OPEN + 5)(lower.close)
        for i in range(PER):
            unit = PER * (m - OPEN) + i
            inside(unit, 0, UNITS, lambda: chain_unit(
                unit, jnp.where(x == 0, z, 4 * PT), q, lead, (w0a, w0b, p0h, p0x), edge, a_ref, u_ref, w_ref, t_ref))
        return carry

    steps = max(4 * NS + 7 * ZL + FL, OPEN + UNITS // PER)
    lax.fori_loop(0, steps, step, 0)
    chain_close(jnp.where(x == 0, z, 4 * PT), q, w1a, w1b, edge, u_ref, w_ref)

    @pl.when(z == q)
    def _():
        right[pl.ds(x, 1)] = left[...][None]

    sides.drain()
    upper.drain()
    lower.drain()

    def tip_sent(i):
        tip(z, i, other).wait_send()

    pl.when(x <= 1)(lambda: tip_sent(0))
    pl.when(x == 0)(lambda: tip_sent(1))
    for i in range(2, 9):
        tip_sent(i)

    def drain(n, carry):
        for par in range(2):
            t, a = 2 * lax.rem(n, 4) + par, n // 4
            def sent(s):
                r = right.at[0, t, a]
                to(r, r, s, s, other).wait_send()

            @pl.when((n < 4 * NS) | (zd[par] == 0))
            def _():
                sent(xs.at[t, a, 0])
                sent(xs.at[t, a, 1])
                sent(rs.at[t, a])

            @pl.when(zd[par] < NZ - 1)
            def _():
                @pl.when(n < 4 * NS)
                def _():
                    sent(zs.at[x, t, a])

                @pl.when(n >= 4 * NS)
                def _():
                    for k in range(NX):
                        sent(zs.at[k, t, a])
        return carry
    lax.fori_loop(0, 4 * NA, drain, 0)

def move(pay):
    V = pl.BlockSpec(memory_space=pltpu.VMEM)
    D = pltpu.SemaphoreType.DMA
    wide = PT * 128
    half = lambda *s: jax.ShapeDtypeStruct(s, BF16)
    shape = lambda *s: jax.ShapeDtypeStruct(s, F32)
    return pl.pallas_call(
        lambda *r: move_kernel(True, *r[:3], r[10], *r[3:10], *r[11:]),
        out_shape=[shape(NTC, NA, PR, 128), shape(NX, NTC, NA, PR, 128)] + [half(HALF, 3 * HALF), half(HALF, 3 * wide), half(wide, wide), half(wide, 2 * wide), half(HALF, 3 * HALF),
                      half(HALF, 3 * wide)] + [shape(128, 128)],
        in_specs=[V], out_specs=[V] * 9,
        scratch_shapes=[pltpu.VMEM((NTC, NTC, PR, 128), F32)] + [pltpu.VMEM((wide, wide), F32)] * 3
        + [pltpu.VMEM((128, 2 * wide), F32)]
        + [D((8, 3)), D((8,)), D((4, 8, 5)), D((8, 5, 2)), D((8, 5)), D((4, 8, 5)), D((9,)), D((8,)),
           D((8, 3)), D((8,)), D((8, 3)), D((8,))],
        compiler_params=pltpu.CompilerParams(collective_id=0, has_side_effects=True, vmem_limit_bytes=60 * 2**20),
    )(pay)

def finish_kernel(pos, marks, left, right, w0a, w0b, p0h, p0x, w1a, w1b, edge, work, out, own, opp):
    r, q = pos[2], pos[1]
    group = pl.program_id(0)
    wide = PT * 128

    def solve(read, count):
        raw = jnp.concatenate(
            [jnp.concatenate([read(m, k)[8:] for k in range(PT)], axis=1) for m in range(count)], axis=0)
        high, low = halves(solve_rows(raw, w0a, w0b))
        coarse = mm(high, p0h[...], NT)
        extra = mm(jnp.concatenate([high, low], axis=1), p0x[...], NT)
        parts = []
        for m in range(count):
            rows = slice(m * 128, (m + 1) * 128)
            row = []
            for k in range(PT):
                lanes = slice(k * 128, (k + 1) * 128)
                piece = read(m, PT + k)
                row.append(piece[8:] - coarse[rows, lanes] - jnp.where(piece[0:1] > 0.5, 0.0, extra[rows, lanes]))
            parts.append(jnp.concatenate(row, axis=1))
        return (high, low), halves(solve_rows(jnp.concatenate(parts, axis=0), w1a, w1b))

    @pl.when(group == 0)
    def _():
        first, second = solve(lambda m, k: left[k, m], NA)
        for i, v in enumerate((first[0], second[0], first[1], second[1])):
            own[:, i * wide:(i + 1) * wide] = v

    first, second = solve(lambda m, k: right[m, k, 0], NX)
    for i, v in enumerate((first[1], second[1], first[0], second[0])):
        opp[:, i * wide:(i + 1) * wide] = v

    def rows_from(g):
        coarse = mm(own[g * 128:, :2 * wide], opp[:, 2 * wide:], NT)
        extra = mm(own[g * 128:, :], opp[...], NT)
        for a in range(NA):
            if a < g:
                out[a] = jnp.zeros((NX, 128, 128), F32)
                continue
            i = a * 32 + r
            rows = slice((a - g) * 128, (a - g + 1) * 128)
            for m in range(NX):
                lanes = slice(m * 128, (m + 1) * 128)
                j = g * 32 + m * 8 + q
                mark = marks[a, g * NX + m]
                tile = work[a, m]
                exact = tile - (coarse[rows, lanes] + extra[rows, lanes])
                rough = tile.astype(BF16).astype(F32) - coarse[rows, lanes]
                rough = rough.astype(BF16).astype(F32)
                value = jnp.where(mark == 1, rough, exact)
                out[a, m] = jnp.where(i >= j, value, 0.0)

    for g in range(NA):
        pl.when(group == g)(lambda g=g: rows_from(g))

    @pl.when(group == 0)
    def _():
        for a in range(NA):
            i = a * 32 + r
            rows = slice(a * 128, (a + 1) * 128)
            value = (own[rows, pl.ds(pl.multiple_of(q * 128, 128), 128)].astype(F32)
                     + own[rows, pl.ds(pl.multiple_of(2 * wide + q * 128, 128), 128)].astype(F32))
            if a == 0:
                value = jnp.where((i < 2 * PT) & (i // PT == q // PT), edge[...], value)
            value = jnp.where(marks[a, 0] == 1, value.astype(BF16).astype(F32), value)
            out[a, 0] = jnp.where(i >= q, value, 0.0)

def finish(pos, marks, left, right, parts, work):
    wide = PT * 128
    S = pl.BlockSpec(memory_space=pltpu.SMEM)
    whole = lambda s: pl.BlockSpec(s, lambda g: (0,) * len(s))
    tiles = pl.BlockSpec((NA, NX, 128, 128), lambda g: (0, g, 0, 0))
    return pl.pallas_call(
        finish_kernel,
        grid=(NA,),
        out_shape=jax.ShapeDtypeStruct(work.shape, F32),
        in_specs=[S, S, whole(left.shape), pl.BlockSpec((NX, NTC, 1, PR, 128), lambda g: (0, 0, g, 0, 0))]
        + [whole(v.shape) for v in parts] + [tiles],
        out_specs=tiles,
        scratch_shapes=[pltpu.VMEM((NA * 128, 4 * wide), BF16), pltpu.VMEM((NX * 128, 4 * wide), BF16)],
        compiler_params=pltpu.CompilerParams(vmem_limit_bytes=60 * 2**20, dimension_semantics=("arbitrary",)),
    )(pos, marks, left, right, *parts, work)

def on_device(matrix, flags):
    x, z, y, c = (lax.axis_index(n) for n in ("x", "z", "y", "c"))
    tiles = matrix.reshape(NA, NA * NX, 128, 128)
    marks = flags.reshape(NA, NA * NX)
    first = marks[:, 0][:, None, None]
    own = tiles[:, 0]
    own = jnp.where(first == 1, lax.reduce_precision(own, 8, 7), own)
    pay = jnp.concatenate([jnp.broadcast_to(first.astype(F32), (NA, 8, 128)), own], axis=1)
    left, right, *parts = move(pay)
    pos = jnp.stack([jnp.where(x == 0, z, 4 * PT), 2 * y + c, 8 * x + z]).astype(jnp.int32)
    return finish(pos, marks, left, right, parts, tiles).reshape(matrix.shape)

def solution(mesh):
    finer = Mesh(mesh.devices.reshape(NX, NZ, NY, 2), ("x", "z", "y", "c"))
    rows, cols = ("x", "z"), ("y", "c")
    return jax.shard_map(
        on_device, mesh=finer, in_specs=(P(None, rows, None, cols, None, None), P(None, rows, None, cols)),
        out_specs=P(None, rows, None, cols, None, None), check_vma=False)
```

```python
import jax
import jax.numpy as jnp
from jax import lax
from jax.experimental import pallas as pl
from jax.experimental.pallas import tpu as pltpu
from jax.sharding import Mesh
from jax.sharding import PartitionSpec as P

F32 = jnp.float32
BF16 = jnp.bfloat16
MESH = pl.DeviceIdType.MESH
PT = 4
HI = lax.Precision.HIGHEST
SUB = 32

def halves(v):
    high = v.astype(BF16)
    return high, (v - high.astype(F32)).astype(BF16)

NT = (((1,), (1,)), ((), ()))
TN = (((0,), (0,)), ((), ()))
NN = (((1,), (0,)), ((), ()))

def mm(a, b, dims):
    return lax.dot_general(a, b, dims, preferred_element_type=F32)

def mm6(a, b, dims):
    return lax.dot_general(a, b, dims, precision=HI, preferred_element_type=F32)

def mm3(a, b, dims):
    return mm(a[0], b[0], dims) + (mm(a[0], b[1], dims) + mm(a[1], b[0], dims))

HALF = PT * 128 // 2

def triple(v, axis):
    h, l = halves(v)
    return jnp.concatenate([h, h, l], axis=axis)

def keep_factor(w, wa, wb):
    h, l = halves(w)
    wa[...] = jnp.concatenate([h[:HALF, :HALF], l[:HALF, :HALF], h[:HALF, :HALF]], axis=1)
    wb[...] = jnp.concatenate([h[HALF:], l[HALF:], h[HALF:]], axis=1)

def solve_rows(raw, wa, wb):
    top = mm(triple(raw[:, :HALF], 1), wa[...], NT)
    return jnp.concatenate([top, mm(triple(raw, 1), wb[...], NT)], axis=1)

def small_inverse(block):
    lanes = block.shape[1]
    cols = []
    for k in range(SUB):
        low = 8 * (k // 8)
        cols.append(jnp.broadcast_to(block[low:, k:k + 1], (SUB - low, lanes)))
    row = lax.broadcasted_iota(jnp.int32, (SUB, lanes), 0)
    lane = lax.broadcasted_iota(jnp.int32, (SUB, lanes), 1)
    right = (row == lane).astype(F32)
    done = []
    for k in range(SUB):
        low = 8 * (k // 8)
        own = cols[k]
        scale = lax.rsqrt(own[k - low:k - low + 1, :])
        factor = own * scale
        solved = right[k - low:k - low + 1, :] * scale
        done.append(solved)
        if k == SUB - 1:
            break
        nxt = 8 * ((k + 1) // 8)
        for m in range(k + 1, SUB):
            base = 8 * (m // 8)
            cols[m] = cols[m] - factor[base - low:, :] * factor[m - low:m - low + 1, :]
        right = right[nxt - low:, :] - factor[nxt - low:, :] * solved
    return jnp.concatenate(done, axis=0)

def factor_unit(kb, s, a_ref, u_ref, w_ref, t_ref):
    n = a_ref.shape[0]
    here = pl.ds(pl.multiple_of(kb * 128, 128), 128)

    @pl.when(s == 0)
    def _():
        row = lax.broadcasted_iota(jnp.int32, (128, n), 0)
        lane = lax.broadcasted_iota(jnp.int32, (128, n), 1)
        t_ref[:, :n] = a_ref[here, :]
        t_ref[:, n:] = (lane == row + kb * 128).astype(F32)

        @pl.when(kb > 0)
        def _():
            left = halves(u_ref[:, here])
            t_ref[:, :n] -= mm3(left, halves(u_ref[...]), TN)
            t_ref[:, n:] -= mm3(left, halves(w_ref[...]), TN)

    rows = pl.ds(pl.multiple_of(s * SUB, SUB), SUB)
    out = pl.ds(pl.multiple_of(kb * 128 + s * SUB, SUB), SUB)
    inv = small_inverse(pltpu.roll(t_ref[rows, here], (128 - s * SUB) % 128, 1))[:, :SUB]
    both = mm6(inv, t_ref[rows, :], NN)
    lane = lax.broadcasted_iota(jnp.int32, (SUB, n), 1)
    row = lax.broadcasted_iota(jnp.int32, (SUB, n), 0) + (kb * 128 + s * SUB)
    u_ref[out, :] = jnp.where(lane >= row, both[:, :n], 0.0)
    w_ref[out, :] = jnp.where(lane <= row, both[:, n:], 0.0)
    left = u_ref[out, here]
    hl, hb = halves(left), halves(both)
    t_ref[...] -= mm(jnp.concatenate([hl[0], hl[0], hl[1]], axis=0), jnp.concatenate([hb[0], hb[1], hb[0]], axis=0), TN)

def tile_of(lead, i, t):
    return lead[t, i, 8:, :]

def symmetric(tile):
    row = lax.broadcasted_iota(jnp.int32, tile.shape, 0)
    lane = lax.broadcasted_iota(jnp.int32, tile.shape, 1)
    return jnp.where(row >= lane, tile, tile.T)

def fill_symmetric(a_ref, tile):
    for i in range(PT):
        for t in range(i + 1):
            here = slice(i * 128, (i + 1) * 128), slice(t * 128, (t + 1) * 128)
            value = tile(i, t)
            if i == t:
                a_ref[here] = symmetric(value)
            else:
                a_ref[here] = value
                a_ref[here[1], here[0]] = value.T

def edge_tile(z, q, first, edge, u):
    @pl.when((z >= first) & (z < first + PT) & (q >= first) & (q <= z))
    def _():
        rows = pl.ds(pl.multiple_of(lax.rem(q, PT) * 128, 128), 128)
        lanes = pl.ds(pl.multiple_of(lax.rem(z, PT) * 128, 128), 128)
        edge[...] = u[rows, lanes].T

def chain_open(lead, edge, a, u, w):
    edge[...] = jnp.zeros_like(edge)
    fill_symmetric(a, lambda i, k: tile_of(lead, i, k))
    u[...] = jnp.zeros_like(u)
    w[...] = jnp.zeros_like(w)

def chain_turn(z, q, lead, w0a, w0b, p0h, p0x, edge, a, u, w):
    edge_tile(z, q, 0, edge, u)
    keep_factor(w[...], w0a, w0b)
    wide = PT * 128
    for i in range(PT):
        rows = slice(i * 128, (i + 1) * 128)
        raw = jnp.concatenate([tile_of(lead, PT + i, k) for k in range(PT)], axis=1)
        high, low = halves(solve_rows(raw, w0a, w0b))
        p0h[rows] = high
        p0x[rows, :wide], p0x[rows, wide:] = low, high

    def updated(i, k):
        hi = slice(i * 128, (i + 1) * 128), slice(k * 128, (k + 1) * 128)
        coarse = mm(p0h[hi[0]], p0h[hi[1]], NT)
        extra = mm(p0h[hi[0]], p0x[hi[1], :wide], NT) + mm(p0x[hi[0], :wide], p0h[hi[1]], NT)
        marked = lead[PT + k, PT + i, 0:1, :] > 0.5
        return tile_of(lead, PT + i, PT + k) - coarse - jnp.where(marked, 0.0, extra)

    fill_symmetric(a, updated)
    u[...] = jnp.zeros_like(u)
    w[...] = jnp.zeros_like(w)

def chain_close(z, q, w1a, w1b, edge, u, w):
    edge_tile(z, q, PT, edge, u)
    keep_factor(w[...], w1a, w1b)

UNITS = 2 * PT * 128 // SUB

def chain_unit(n, z, q, lead, outs, edge, a, u, w, t):
    half = UNITS // 2

    @pl.when(n == half)
    def _():
        chain_turn(z, q, lead, *outs[:4], edge, a, u, w)
    k = lax.rem(n, half)
    factor_unit(k // (128 // SUB), lax.rem(k, 128 // SUB), a, u, w, t)

NX, NZ, NY, NA, NTC = 4, 8, 4, 5, 8
PR = 136
ZL, RL, FL, OFF = 1, 2, 4, 4
NS = 4
OPEN = 7
EARLY = 2
PER = 2

def move_kernel(with_chain, pay_ref, left, right, lead, w0a, w0b, p0h, p0x, w1a, w1b, edge,
                a_ref, u_ref, w_ref, t_ref, ls, lr, zs, xs, rs, rr, qs, qr, gs, gr, hs, hr, es, er):
    x, z, y, c = (lax.axis_index(n) for n in ("x", "z", "y", "c"))
    q = 2 * y + c
    xp, xm, xfar = lax.rem(x + 1, NX), lax.rem(x + NX - 1, NX), lax.rem(x + 2, NX)
    zp, zm = lax.rem(z + 1, NZ), lax.rem(z + NZ - 1, NZ)
    yp, ym, yo = lax.rem(y + 1, NY), lax.rem(y + NY - 1, NY), lax.rem(y + 2, NY)
    other = {"c": 1 - c}

    def to(src, dst, send, recv, where):
        return pltpu.make_async_remote_copy(src_ref=src, dst_ref=dst, send_sem=send, recv_sem=recv,
                                            device_id=where, device_id_type=MESH)

    barrier = pltpu.get_barrier_semaphore()
    peers = [{"x": xp}, {"x": xm}, {"z": zp}, {"z": zm}, {"y": yp}, {"y": ym}, other]
    for p in peers:
        pl.semaphore_signal(barrier, inc=1, device_id=p, device_id_type=MESH)
    pl.semaphore_wait(barrier, len(peers))

    class Gather:
        def __init__(self, own, slot, send, recv, limit):
            self.own, self.slot, self.send, self.recv, self.limit = own, slot, send, recv, limit

        def on(self, k, fn):
            if self.limit == NTC:
                fn()
            else:
                pl.when(k < self.limit)(fn)

        def copy(self, src, k, i, where):
            return to(src, self.slot(k), self.send.at[k, i], self.recv.at[k], where)

        def got(self, k):
            self.copy(self.slot(k), k, 0, other).wait_recv()

        def open(self):
            def go():
                for i, where in enumerate(({"y": yp}, {"y": ym}, other)):
                    self.copy(self.own, q, i, where).start()
            self.on(q, go)

        def pass_on(self):
            for k, core, where in ((2 * ym + c, 0, {"y": yp}), (2 * yp + c, 1, {"y": ym})):
                def go(k=k, core=core, where=where):
                    self.got(k)
                    @pl.when(c == core)
                    def _():
                        self.copy(self.slot(k), k, 0, where).start()
                    self.copy(self.slot(k), k, 2, other).start()
                self.on(k, go)

        def share(self):
            k = 2 * yo + c
            def go():
                self.got(k)
                self.copy(self.slot(k), k, 2, other).start()
            self.on(k, go)

        def close(self):
            for n in range(NY):
                k = 2 * n + 1 - c
                self.on(k, lambda k=k: self.got(k))

        def drain(self):
            def sent(k, i):
                self.copy(self.slot(k), k, i, other).wait_send()
            self.on(q, lambda: [sent(q, i) for i in range(3)] and None)
            for k, core in ((2 * ym + c, 0), (2 * yp + c, 1)):
                def go(k=k, core=core):
                    pl.when(c == core)(lambda: sent(k, 0))
                    sent(k, 2)
                self.on(k, go)
            self.on(2 * yo + c, lambda: sent(2 * yo + c, 2))

    first, rest = pl.ds(0, EARLY), pl.ds(EARLY, NA - EARLY)
    sides = Gather(pay_ref.at[first], lambda k: left.at[k, first], ls, lr, NTC)
    later = Gather(pay_ref.at[rest], lambda k: left.at[k, rest], es, er, NTC)
    upper = Gather(lead.at[q, pl.ds(0, PT)], lambda k: lead.at[k, pl.ds(0, PT)], gs, gr, PT)
    lower = Gather(lead.at[q, pl.ds(PT, PT)], lambda k: lead.at[k, pl.ds(PT, PT)], hs, hr, NTC)

    sides.open()
    later.open()

    mine = pay_ref.at[0]
    def tip(row, send, where, src=None):
        slot = lead.at[q, row]
        return to(slot if src is None else src, slot, qs.at[send], qr.at[row], where)

    @pl.when(x == 0)
    def _():
        tip(z, 0, {"x": xp}, mine).start()
        tip(z, 1, {"x": xm}, mine).start()
        lead[pl.ds(q, 1), pl.ds(z, 1)] = pay_ref[0][None, None]
        tip(z, 2, {"z": zp}, mine).start()
        tip(z, 6, {"z": zm}, mine).start()

    @pl.when(x > 0)
    def _():
        tip(z, 0, other).wait_recv()
        @pl.when(x == 1)
        def _():
            tip(z, 0, {"x": xp}).start()
        tip(z, 2, {"z": zp}).start()
        tip(z, 6, {"z": zm}).start()

    def ring(h):
        row = lax.rem(z - h + NZ, NZ)
        tip(row, 0, other).wait_recv()
        if h < 4:
            tip(row, 2 + h, {"z": zp}).start()
            row = lax.rem(z + h, NZ)
            tip(row, 0, other).wait_recv()
            if h < 3:
                tip(row, 6 + h, {"z": zm}).start()

    sides.pass_on()
    sides.share()
    sides.close()
    left[pl.ds(q, 1)] = pay_ref[...][None]

    zd = (lax.rem(z - q + NZ, NZ), lax.rem(q - z + NZ, NZ))
    znext = ({"z": zp}, {"z": zm})
    xnext = ({"x": xp}, {"x": xm})
    xprev = (xm, xp)

    def landed(src, t, a):
        r = right.at[src, t, a]
        to(r, r, rs.at[t, a], rr.at[src, t, a], other).wait_recv()

    def push(src, t, a, send, where, ref=None):
        r = right.at[src, t, a]
        to(r if ref is None else ref, r, send, rr.at[src, t, a], where).start()

    def inside(n, low, high, fn):
        pl.when((n >= low) & (n < high))(fn)

    def near(par, n):
        t, a = 2 * lax.rem(n, 4) + par, n // 4

        def send(ref):
            @pl.when(zd[par] < NZ - 1)
            def _():
                push(x, t, a, zs.at[x, t, a], znext[par], ref)
            push(x, t, a, xs.at[t, a, 0], {"x": xp}, ref)
            push(x, t, a, xs.at[t, a, 1], {"x": xm}, ref)

        @pl.when(zd[par] == 0)
        def _():
            send(left.at[t, a])

        @pl.when(zd[par] > 0)
        def _():
            landed(x, t, a)
            send(None)

    def relay(par, n):
        t, a = 2 * lax.rem(n, 4) + par, n // 4
        landed(xprev[par], t, a)
        push(xprev[par], t, a, rs.at[t, a], xnext[par])

    def last_landed(par, n):
        t, a = 2 * lax.rem(n, 4) + par, n // 4
        landed(xprev[1 - par], t, a)
        landed(xfar, t, a)

    def spread(par, n):
        t, a = 2 * lax.rem(n, 4) + par, n // 4
        push(x, t, a, xs.at[t, a, 0], {"x": xp}, left.at[t, a])
        push(x, t, a, xs.at[t, a, 1], {"x": xm}, left.at[t, a])

    far = 4 * (NA - NS)

    def stream(par, k):
        rel, j = k // far, lax.rem(k, far)
        t, a = 2 * lax.rem(j, 4) + par, NS + j // 4
        sign = 3 if par == 0 else 1
        src = lax.rem(x + jnp.where(rel == 0, 0, jnp.where(rel == 1, sign, jnp.where(rel == 2, 4 - sign, 2))), NX)

        @pl.when((zd[par] > 0) | (rel > 1))
        def _():
            landed(src, t, a)

        @pl.when(zd[par] < NZ - 1)
        def _():
            own = (zd[par] == 0) & (rel == 0)
            @pl.when(own)
            def _():
                push(src, t, a, zs.at[src, t, a], znext[par], left.at[t, a])

            @pl.when(jnp.logical_not(own))
            def _():
                push(src, t, a, zs.at[src, t, a], znext[par])

    def step(m, carry):
        for par in range(2):
            n = m - zd[par] * ZL
            inside(n, 0, 4 * NS, lambda: near(par, n))
            @pl.when((zd[par] == 0) & (n >= OFF) & (n < far // 2 + OFF))
            def _():
                spread(par, 4 * NS + 2 * (n - OFF))
                spread(par, 4 * NS + 2 * (n - OFF) + 1)
            inside(n - RL, 0, 4 * NS, lambda: relay(par, n - RL))
            @pl.when((zd[par] == 0) & (n >= OFF + RL) & (n < far // 2 + OFF + RL))
            def _():
                relay(par, 4 * NS + 2 * (n - OFF - RL))
                relay(par, 4 * NS + 2 * (n - OFF - RL) + 1)
            for i in range(2):
                k = 2 * (n - OFF) + i
                inside(k, 0, NX * far, lambda: stream(par, k))
            inside(n - FL, 0, 4 * NS, lambda: last_landed(par, n - FL))
        for h in range(1, 5):
            pl.when(m == h - 1)(lambda h=h: ring(h))
        pl.when(m == 1)(later.pass_on)
        pl.when(m == 2)(later.share)
        @pl.when(m == 3)
        def _():
            later.close()
            upper.open()
            lower.open()
        pl.when(m == OPEN - 2)(upper.pass_on)
        @pl.when(m == OPEN)
        def _():
            upper.share()
            upper.close()
            chain_open(lead, edge, a_ref, u_ref, w_ref)
        pl.when(m == OPEN + 1)(lower.pass_on)
        pl.when(m == OPEN + 3)(lower.share)
        pl.when(m == OPEN + 5)(lower.close)
        for i in range(PER):
            unit = PER * (m - OPEN) + i
            inside(unit, 0, UNITS, lambda: chain_unit(
                unit, jnp.where(x == 0, z, 4 * PT), q, lead, (w0a, w0b, p0h, p0x), edge, a_ref, u_ref, w_ref, t_ref))
        return carry

    steps = max(4 * NS + 7 * ZL + FL, OPEN + UNITS // PER)
    lax.fori_loop(0, steps, step, 0)
    chain_close(jnp.where(x == 0, z, 4 * PT), q, w1a, w1b, edge, u_ref, w_ref)

    @pl.when(z == q)
    def _():
        right[pl.ds(x, 1)] = left[...][None]

    sides.drain()
    later.drain()
    upper.drain()
    lower.drain()

    def tip_sent(i):
        tip(z, i, other).wait_send()

    pl.when(x <= 1)(lambda: tip_sent(0))
    pl.when(x == 0)(lambda: tip_sent(1))
    for i in range(2, 9):
        tip_sent(i)

    def drain(n, carry):
        for par in range(2):
            t, a = 2 * lax.rem(n, 4) + par, n // 4
            def sent(s):
                r = right.at[0, t, a]
                to(r, r, s, s, other).wait_send()

            @pl.when((n < 4 * NS) | (zd[par] == 0))
            def _():
                sent(xs.at[t, a, 0])
                sent(xs.at[t, a, 1])
                sent(rs.at[t, a])

            @pl.when(zd[par] < NZ - 1)
            def _():
                @pl.when(n < 4 * NS)
                def _():
                    sent(zs.at[x, t, a])

                @pl.when(n >= 4 * NS)
                def _():
                    for k in range(NX):
                        sent(zs.at[k, t, a])
        return carry
    lax.fori_loop(0, 4 * NA, drain, 0)

def move(pay):
    V = pl.BlockSpec(memory_space=pltpu.VMEM)
    D = pltpu.SemaphoreType.DMA
    wide = PT * 128
    half = lambda *s: jax.ShapeDtypeStruct(s, BF16)
    shape = lambda *s: jax.ShapeDtypeStruct(s, F32)
    return pl.pallas_call(
        lambda *r: move_kernel(True, *r[:3], r[10], *r[3:10], *r[11:]),
        out_shape=[shape(NTC, NA, PR, 128), shape(NX, NTC, NA, PR, 128)] + [half(HALF, 3 * HALF), half(HALF, 3 * wide), half(wide, wide), half(wide, 2 * wide), half(HALF, 3 * HALF),
                      half(HALF, 3 * wide)] + [shape(128, 128)],
        in_specs=[V], out_specs=[V] * 9,
        scratch_shapes=[pltpu.VMEM((NTC, NTC, PR, 128), F32)] + [pltpu.VMEM((wide, wide), F32)] * 3
        + [pltpu.VMEM((128, 2 * wide), F32)]
        + [D((8, 3)), D((8,)), D((4, 8, 5)), D((8, 5, 2)), D((8, 5)), D((4, 8, 5)), D((9,)), D((8,)),
           D((8, 3)), D((8,)), D((8, 3)), D((8,)), D((8, 3)), D((8,))],
        compiler_params=pltpu.CompilerParams(collective_id=0, has_side_effects=True, vmem_limit_bytes=60 * 2**20),
    )(pay)

def finish_kernel(pos, marks, left, right, w0a, w0b, p0h, p0x, w1a, w1b, edge, work, out, own, opp):
    r, q = pos[2], pos[1]
    group = pl.program_id(0)
    wide = PT * 128

    def solve(read, count):
        raw = jnp.concatenate(
            [jnp.concatenate([read(m, k)[8:] for k in range(PT)], axis=1) for m in range(count)], axis=0)
        high, low = halves(solve_rows(raw, w0a, w0b))
        coarse = mm(high, p0h[...], NT)
        extra = mm(jnp.concatenate([high, low], axis=1), p0x[...], NT)
        parts = []
        for m in range(count):
            rows = slice(m * 128, (m + 1) * 128)
            row = []
            for k in range(PT):
                lanes = slice(k * 128, (k + 1) * 128)
                piece = read(m, PT + k)
                row.append(piece[8:] - coarse[rows, lanes] - jnp.where(piece[0:1] > 0.5, 0.0, extra[rows, lanes]))
            parts.append(jnp.concatenate(row, axis=1))
        return (high, low), halves(solve_rows(jnp.concatenate(parts, axis=0), w1a, w1b))

    @pl.when(group == 0)
    def _():
        first, second = solve(lambda m, k: left[k, m], NA)
        for i, v in enumerate((first[0], second[0], first[1], second[1])):
            own[:, i * wide:(i + 1) * wide] = v

    first, second = solve(lambda m, k: right[m, k, 0], NX)
    for i, v in enumerate((first[1], second[1], first[0], second[0])):
        opp[:, i * wide:(i + 1) * wide] = v

    def rows_from(g):
        coarse = mm(own[g * 128:, :2 * wide], opp[:, 2 * wide:], NT)
        extra = mm(own[g * 128:, :], opp[...], NT)
        for a in range(NA):
            if a < g:
                out[a] = jnp.zeros((NX, 128, 128), F32)
                continue
            i = a * 32 + r
            rows = slice((a - g) * 128, (a - g + 1) * 128)
            for m in range(NX):
                lanes = slice(m * 128, (m + 1) * 128)
                j = g * 32 + m * 8 + q
                mark = marks[a, g * NX + m]
                tile = work[a, m]
                exact = tile - (coarse[rows, lanes] + extra[rows, lanes])
                rough = tile.astype(BF16).astype(F32) - coarse[rows, lanes]
                rough = rough.astype(BF16).astype(F32)
                value = jnp.where(mark == 1, rough, exact)
                out[a, m] = jnp.where(i >= j, value, 0.0)

    for g in range(NA):
        pl.when(group == g)(lambda g=g: rows_from(g))

    @pl.when(group == 0)
    def _():
        for a in range(NA):
            i = a * 32 + r
            rows = slice(a * 128, (a + 1) * 128)
            value = (own[rows, pl.ds(pl.multiple_of(q * 128, 128), 128)].astype(F32)
                     + own[rows, pl.ds(pl.multiple_of(2 * wide + q * 128, 128), 128)].astype(F32))
            if a == 0:
                value = jnp.where((i < 2 * PT) & (i // PT == q // PT), edge[...], value)
            value = jnp.where(marks[a, 0] == 1, value.astype(BF16).astype(F32), value)
            out[a, 0] = jnp.where(i >= q, value, 0.0)

def finish(pos, marks, left, right, parts, work):
    wide = PT * 128
    S = pl.BlockSpec(memory_space=pltpu.SMEM)
    whole = lambda s: pl.BlockSpec(s, lambda g: (0,) * len(s))
    tiles = pl.BlockSpec((NA, NX, 128, 128), lambda g: (0, g, 0, 0))
    return pl.pallas_call(
        finish_kernel,
        grid=(NA,),
        out_shape=jax.ShapeDtypeStruct(work.shape, F32),
        in_specs=[S, S, whole(left.shape), pl.BlockSpec((NX, NTC, 1, PR, 128), lambda g: (0, 0, g, 0, 0))]
        + [whole(v.shape) for v in parts] + [tiles],
        out_specs=tiles,
        scratch_shapes=[pltpu.VMEM((NA * 128, 4 * wide), BF16), pltpu.VMEM((NX * 128, 4 * wide), BF16)],
        compiler_params=pltpu.CompilerParams(vmem_limit_bytes=60 * 2**20, dimension_semantics=("arbitrary",)),
    )(pos, marks, left, right, *parts, work)

def on_device(matrix, flags):
    x, z, y, c = (lax.axis_index(n) for n in ("x", "z", "y", "c"))
    tiles = matrix.reshape(NA, NA * NX, 128, 128)
    marks = flags.reshape(NA, NA * NX)
    first = marks[:, 0][:, None, None]
    own = tiles[:, 0]
    own = jnp.where(first == 1, lax.reduce_precision(own, 8, 7), own)
    pay = jnp.concatenate([jnp.broadcast_to(first.astype(F32), (NA, 8, 128)), own], axis=1)
    left, right, *parts = move(pay)
    pos = jnp.stack([jnp.where(x == 0, z, 4 * PT), 2 * y + c, 8 * x + z]).astype(jnp.int32)
    return finish(pos, marks, left, right, parts, tiles).reshape(matrix.shape)

def solution(mesh):
    finer = Mesh(mesh.devices.reshape(NX, NZ, NY, 2), ("x", "z", "y", "c"))
    rows, cols = ("x", "z"), ("y", "c")
    return jax.shard_map(
        on_device, mesh=finer, in_specs=(P(None, rows, None, cols, None, None), P(None, rows, None, cols)),
        out_specs=P(None, rows, None, cols, None, None), check_vma=False)
```
